32 devices in a mesh: aa: 4 (over y, x), ba: 2 (over core), col: 4 (over z).
Axes of the slice: x: 2, y: 2, z: 4, core: 2. Of those that a mesh axis runs over, the one named last changes fastest.
Arguments:
- tokens: bfloat16 [1024, 7168], P('aa', ('ba', 'col')), may hold values from -6 to 6
- expert_ids: int32 [1024, 8], P('aa'), may hold values from 0 to 383, as said below
- route_weight: float32 [1024, 8], P('aa'), may hold values from 0.5 to 2
- w_gate: bfloat16 [4, 7168, 2048], P('aa', None, ('ba', 'col')), may hold values from -0.0625 to 0.0625
- w_up: bfloat16 [4, 7168, 2048], P('aa', None, ('ba', 'col')), may hold values from -0.0625 to 0.0625
- w_down: bfloat16 [4, 2048, 7168], P('aa', ('ba', 'col')), may hold values from -0.125 to 0.125
Outputs:
- mixed: bfloat16 [1024, 7168], P('aa', ('ba', 'col'))
The draws below stay inside these ranges and needn't reach their ends.
Inputs may be any that keep to these rules, and one draw needn't show every extreme that they name: `expert_ids`: each row names 8 different experts.
All inputs are finite; a program needn't handle non-finite values.
Results may differ from the reference program's by a relative error of at most 0.015.
Values may be sent and summed in bfloat16 or wider, within the bound.
A program may use at most 64 MiB of HBM per device.

```python
import jax
import jax.numpy as jnp
from jax import lax

D = 7168
FF = 2048
EXPERTS = 384
TOP = 8
TOK_AA = 256
CAP = 8
EXPERTS_COMPUTED = 4
TOKENS = 1024
N_AA = 4
N_BA = 2
N_COL = 4


def draw_expert_ids(key, part):
    first = jax.random.fold_in(key, 11)
    second = jax.random.fold_in(key, 23)
    even_share = jax.random.randint(first, (TOKENS, EXPERTS), 0, 2 ** 20, dtype=jnp.int32)
    expert_numbering = jnp.arange(EXPERTS, dtype=jnp.int32)
    expert_popularity = jax.random.randint(second, (EXPERTS,), 0, 4, dtype=jnp.int32)
    extra_logit = jnp.where(expert_numbering < EXPERTS_COMPUTED, expert_popularity * 2 ** 23, 0).astype(jnp.int32)
    router_logits = even_share * 1024 + expert_numbering[None, :] + extra_logit[None, :]
    picked = lax.top_k(router_logits, TOP)[1]
    return picked.astype(jnp.int32)


def steps_of(own_key, shape, shards, least, top_value):
    level = 1.0
    for dim, parts in shards:
        heights = jax.random.uniform(jax.random.fold_in(jax.random.fold_in(own_key, 6), dim), (parts,), jnp.float32, least / len(shards), top_value / len(shards))
        level = level * jnp.repeat(jnp.exp(heights), shape[dim] // parts).reshape((-1,) + (1,) * (len(shape) - 1 - dim))
    return level


def gaussian(stream_key, shape, spread, reach, split=(), kind=jnp.bfloat16):
    array = spread * jax.random.normal(stream_key, shape, jnp.float32)
    if split:
        array = array * steps_of(stream_key, shape, split, -0.22, 0.18)
    return jnp.clip(array, -reach, reach).astype(kind)


def setup_inputs(seed: int = 0) -> dict:
    key_of = jax.random.split(jax.random.key(seed), 7)
    tokens = gaussian(key_of[0], (TOKENS, D), 1.0, 6.0, ((0, 4), (1, 8)))
    expert_ids = draw_expert_ids(jax.random.fold_in(key_of[6], 71), 0)
    route_weight = jnp.clip(0.5 + 1.5 * jax.random.uniform(key_of[2], (TOKENS, TOP), jnp.float32) ** steps_of(key_of[2], (TOKENS, TOP), ((0, 4),), -0.2, 0.2), 0.5, 2.0)
    w_gate = gaussian(key_of[3], (EXPERTS_COMPUTED, D, FF), D ** -0.5, 0.0625, ((0, 4), (2, 8)))
    w_up = gaussian(key_of[4], (EXPERTS_COMPUTED, D, FF), D ** -0.5, 0.0625, ((0, 4), (2, 8)))
    w_down = gaussian(key_of[5], (EXPERTS_COMPUTED, FF, D), FF ** -0.5, 0.125, ((0, 4), (1, 8)))
    return {"tokens": tokens, "expert_ids": expert_ids, "route_weight": route_weight, "w_gate": w_gate, "w_up": w_up, "w_down": w_down}


def assign(group_ids):
    expert_pool = jnp.arange(EXPERTS_COMPUTED, dtype=jnp.int32)
    matched = group_ids[:, :, None] == expert_pool[None, None, :]
    counted = jnp.sum(matched.astype(jnp.int32), axis=1)
    before = jnp.cumsum(counted, axis=0) - counted
    retained = (counted > 0) & (before < CAP)
    placed = retained[:, :, None] & (before[:, :, None] == jnp.arange(CAP, dtype=jnp.int32)[None, None, :])
    positions = jnp.arange(TOK_AA, dtype=jnp.int32)[:, None, None]
    source_row = jnp.sum(jnp.where(placed, positions, 0), axis=0).astype(jnp.int32)
    filled = jnp.any(placed, axis=0)
    pick_slot = jnp.sum(jnp.where(matched, before[:, None, :], 0), axis=2).astype(jnp.int32)
    pick_kept = jnp.any(matched & retained[:, None, :], axis=2)
    return source_row, filled, pick_slot, pick_kept


def expert_ffn(operands):
    rows, gate_matrix, up_matrix, down_matrix = operands
    gate_sum = jnp.dot(rows, gate_matrix, preferred_element_type=jnp.float32)
    up_sum = jnp.dot(rows, up_matrix, preferred_element_type=jnp.float32)
    hidden = (jax.nn.silu(gate_sum) * up_sum).astype(jnp.bfloat16)
    blocks = N_BA * N_COL
    width = FF // blocks
    total = jnp.zeros((rows.shape[0], D), jnp.float32)
    for segment in range(blocks):
        partial_value = jnp.dot(hidden[:, segment * width:(segment + 1) * width],
                          down_matrix[segment * width:(segment + 1) * width],
                          preferred_element_type=jnp.float32).astype(jnp.bfloat16)
        partial_value = lax.optimization_barrier(partial_value)
        total = total + partial_value.astype(jnp.float32)
    return total.astype(jnp.bfloat16)


def reference(tokens, expert_ids, route_weight, w_gate, w_up, w_down):
    grouped = tokens.reshape(N_AA, TOK_AA, D)
    source_row, filled, pick_slot, pick_kept = jax.vmap(assign)(expert_ids.reshape(N_AA, TOK_AA, TOP))
    group_index = jnp.arange(N_AA, dtype=jnp.int32)[:, None, None]
    rows = grouped[group_index, source_row]
    rows = jnp.where(filled[:, :, :, None], rows, jnp.zeros_like(rows))
    per_expert = jnp.transpose(rows, (1, 0, 2, 3)).reshape(EXPERTS_COMPUTED, N_AA * CAP, D)
    outputs = lax.map(expert_ffn, (per_expert, w_gate, w_up, w_down)).reshape(EXPERTS_COMPUTED, N_AA, CAP, D)
    target = jnp.clip(expert_ids, 0, EXPERTS_COMPUTED - 1).astype(jnp.int32)
    slots = pick_slot.reshape(TOKENS, TOP)
    kept_flat = pick_kept.reshape(TOKENS, TOP)
    group_of = (jnp.arange(TOKENS, dtype=jnp.int32) // TOK_AA).astype(jnp.int32)
    weights = jnp.where(kept_flat, route_weight, jnp.zeros_like(route_weight))
    mixed = jnp.zeros((TOKENS, D), jnp.float32)
    for pick in range(TOP):
        chosen = outputs[target[:, pick], group_of, slots[:, pick]].astype(jnp.float32)
        mixed = mixed + weights[:, pick, None] * chosen
    return mixed.astype(jnp.bfloat16)
```

```python
import functools

import jax
import jax.numpy as jnp
from jax import lax
from jax.experimental import pallas as pl
from jax.experimental.pallas import tpu as pltpu
from jax.sharding import PartitionSpec as P

CAP = 8
MESH = pl.DeviceIdType.MESH
F32 = jnp.float32
BF16 = jnp.bfloat16


def kernel(
    E, B, Z,
    ids_hbm, rw_hbm, tok_hbm, wg_hbm, wu_hbm, wd_hbm,
    merged_ref, wt_ref,
    ids, rw, tok, wg, wu, wd, disp, xr, acc_g, acc_u, part, pr, total, rr,
    in_sem, wg_sem, wu_sem, wd_sem,
    d_send, d_recv, f_send, f_recv, p_send, p_recv, r_send, r_recv,
):
    a = lax.axis_index("aa")
    c = lax.axis_index("ba")
    z = lax.axis_index("col")
    N = B * Z
    T = tok.shape[0]
    W = tok.shape[1]
    rows = E * CAP

    def far_first():
        order = []
        for k in sorted(range(Z), key=lambda k: -min(k, Z - k)):
            for i in range(E):
                if (k, i) != (0, 0):
                    order.append((k, i))
        return order

    def at(k, n, base):
        return lax.rem(base + k, n)

    ins = [
        pltpu.make_async_copy(ids_hbm, ids, in_sem.at[0]),
        pltpu.make_async_copy(rw_hbm, rw, in_sem.at[1]),
        pltpu.make_async_copy(tok_hbm, tok, in_sem.at[2]),
    ]
    for copy in ins:
        copy.start()

    barrier = pltpu.get_barrier_semaphore()
    for k, i in far_first():
        pl.semaphore_signal(
            barrier, inc=1, device_id=(at(i, E, a), c, at(k, Z, z)), device_id_type=MESH
        )
    for b in range(1, B):
        pl.semaphore_signal(barrier, inc=1, device_id=(a, at(b, B, c), z), device_id_type=MESH)

    chunks = [(at(b, B, c), at(k, Z, z)) for k in range(Z) for b in range(B)]
    w_copies = []
    for cc, zz in chunks:
        j = cc * Z + zz
        span = pl.ds(pl.multiple_of(j * W, 128), W)
        for src, dst, sem in ((wg_hbm, wg, wg_sem), (wu_hbm, wu, wu_sem)):
            pltpu.make_async_copy(src.at[0, span, :], dst.at[j], sem.at[j]).start()
    for cc, zz in chunks:
        j = cc * Z + zz
        span = pl.ds(pl.multiple_of(j * W, 128), W)
        pltpu.make_async_copy(wd_hbm.at[0, :, span], wd.at[j], wd_sem.at[j]).start()

    ins[0].wait()
    ins[1].wait()
    expert = lax.broadcasted_iota(jnp.int32, (E, T), 0)
    counted = jnp.zeros((E, T), F32)
    shares = jnp.zeros((E, T), F32)
    for k in range(ids.shape[0]):
        match = jnp.broadcast_to(ids[k : k + 1, :], (E, T)) == expert
        counted = counted + jnp.where(match, 1.0, 0.0)
        shares = shares + jnp.where(match, jnp.broadcast_to(rw[k : k + 1, :], (E, T)), 0.0)
    earlier = lax.broadcasted_iota(jnp.int32, (T, T), 0) < lax.broadcasted_iota(
        jnp.int32, (T, T), 1
    )
    before = jnp.dot(
        counted.astype(BF16), jnp.where(earlier, 1.0, 0.0).astype(BF16), preferred_element_type=F32
    )
    slot = lax.broadcasted_iota(jnp.int32, (CAP, T), 0).astype(F32)
    placed = []
    weights = []
    for e in range(E):
        hit = jnp.broadcast_to(counted[e : e + 1, :], (CAP, T)) > 0.0
        rank = jnp.broadcast_to(before[e : e + 1, :], (CAP, T))
        one = jnp.where(hit & (rank == slot), 1.0, 0.0)
        placed.append(one)
        weights.append(one * jnp.broadcast_to(shares[e : e + 1, :], (CAP, T)))
    chooser = jnp.concatenate(placed, axis=0).astype(BF16)

    ins[2].wait()
    picked = jnp.dot(chooser, tok[...], preferred_element_type=F32)
    for e in range(E):
        disp[e] = picked[e * CAP : (e + 1) * CAP, :].astype(BF16)
    mine = c * Z + z
    xr[mine, a] = disp[a]

    pl.semaphore_wait(barrier, E * Z - 1 + B - 1)

    sends = []
    for k, i in far_first():
        aa, zz = at(i, E, a), at(k, Z, z)
        copy = pltpu.make_async_remote_copy(
            src_ref=disp.at[aa], dst_ref=xr.at[mine, a],
            send_sem=d_send.at[zz, aa], recv_sem=d_recv.at[z, a],
            device_id=(aa, c, zz), device_id_type=MESH,
        )
        copy.start()
        sends.append(copy)

    weight = jnp.concatenate(weights, axis=0)
    high = weight.astype(BF16)
    low = (weight - high.astype(F32)).astype(BF16)
    wt_ref[...] = jnp.concatenate([high, low], axis=0)

    acc_g[...] = jnp.zeros_like(acc_g)
    acc_u[...] = jnp.zeros_like(acc_u)

    def feed(j):
        span = pl.ds(pl.multiple_of(j * W, 128), W)
        x = xr[j].astype(F32).reshape(rows, W).astype(BF16)
        pltpu.make_async_copy(wg_hbm.at[0, span, :], wg.at[j], wg_sem.at[j]).wait()
        pltpu.make_async_copy(wu_hbm.at[0, span, :], wu.at[j], wu_sem.at[j]).wait()
        acc_g[...] += jnp.dot(x, wg[j], preferred_element_type=F32)
        acc_u[...] += jnp.dot(x, wu[j], preferred_element_type=F32)

    def feed_forwarded(k):
        zz = at(k, Z, z)
        for b in range(1, B):
            j = at(B - b, B, c) * Z + zz
            pltpu.make_async_remote_copy(
                src_ref=xr.at[j], dst_ref=xr.at[j],
                send_sem=f_send.at[b - 1, zz], recv_sem=f_recv.at[b - 1, zz],
                device_id=(a, at(b, B, c), z), device_id_type=MESH,
            ).wait_recv()
            feed(j)

    for k in range(Z):
        zz = at(k, Z, z)
        j = c * Z + zz
        for i in range(E):
            if (k, i) != (0, 0):
                aa = at(i, E, a)
                pltpu.make_async_remote_copy(
                    src_ref=xr.at[j, aa], dst_ref=xr.at[j, aa],
                    send_sem=d_send.at[zz, aa], recv_sem=d_recv.at[zz, aa],
                    device_id=(a, at(1, B, c), z), device_id_type=MESH,
                ).wait_recv()
        for b in range(1, B):
            copy = pltpu.make_async_remote_copy(
                src_ref=xr.at[j], dst_ref=xr.at[j],
                send_sem=f_send.at[b - 1, zz], recv_sem=f_recv.at[b - 1, zz],
                device_id=(a, at(b, B, c), z), device_id_type=MESH,
            )
            copy.start()
            sends.append(copy)
        feed(j)
        if k > 0:
            feed_forwarded(k - 1)
    feed_forwarded(Z - 1)

    gate = acc_g[...]
    hidden = (gate / (1.0 + jnp.exp(-gate)) * acc_u[...]).astype(BF16)

    def down(j):
        span = pl.ds(pl.multiple_of(j * W, 128), W)
        pltpu.make_async_copy(wd_hbm.at[0, :, span], wd.at[j], wd_sem.at[j]).wait()
        return jnp.dot(hidden, wd[j], preferred_element_type=F32)

    z_order = sorted(range(Z), key=lambda k: -min(k, Z - k))
    for k in z_order:
        zz = at(k, Z, z)
        for b in range(1, B):
            cc = at(b, B, c)
            part[b - 1, zz] = down(cc * Z + zz).astype(BF16)
            copy = pltpu.make_async_remote_copy(
                src_ref=part.at[b - 1, zz], dst_ref=pr.at[b - 1, zz],
                send_sem=p_send.at[b - 1, zz], recv_sem=p_recv.at[b - 1, zz],
                device_id=(a, cc, z), device_id_type=MESH,
            )
            copy.start()
            sends.append(copy)
    for k in z_order:
        zz = at(k, Z, z)
        value = down(c * Z + zz)
        for b in range(1, B):
            pltpu.make_async_remote_copy(
                src_ref=part.at[b - 1, zz], dst_ref=pr.at[b - 1, zz],
                send_sem=p_send.at[b - 1, zz], recv_sem=p_recv.at[b - 1, zz],
                device_id=(a, at(b, B, c), z), device_id_type=MESH,
            ).wait_recv()
            value = value + pr[b - 1, zz].astype(F32)
        for e in range(E):
            total[zz, e] = value[e * CAP : (e + 1) * CAP, :].astype(BF16)
        for i in range(E):
            aa = at(i, E, a)
            if (k, i) == (0, 0):
                rr[a, z] = total[z, a]
                continue
            copy = pltpu.make_async_remote_copy(
                src_ref=total.at[zz, aa], dst_ref=rr.at[a, z],
                send_sem=r_send.at[zz, aa], recv_sem=r_recv.at[a, z],
                device_id=(aa, c, zz), device_id_type=MESH,
            )
            copy.start()
            sends.append(copy)

    for k in range(Z):
        for i in range(E):
            if (k, i) != (0, 0):
                aa, zz = at(i, E, a), at(k, Z, z)
                pltpu.make_async_remote_copy(
                    src_ref=rr.at[aa, zz], dst_ref=rr.at[aa, zz],
                    send_sem=r_send.at[zz, aa], recv_sem=r_recv.at[aa, zz],
                    device_id=(a, at(1, B, c), z), device_id_type=MESH,
                ).wait_recv()
    outs = []
    for e in range(E):
        value = rr[e, 0].astype(F32)
        for k in range(1, Z):
            value = value + rr[e, k].astype(F32)
        outs.append(value)
    merged = jnp.concatenate(outs, axis=0).astype(BF16)
    merged_ref[0:rows, :] = merged
    merged_ref[rows : 2 * rows, :] = merged
    for copy in sends:
        copy.wait_send()


def shards(E, B, Z, tokens, expert_ids, route_weight, w_gate, w_up, w_down):
    T, W = tokens.shape
    H = w_gate.shape[2]
    N = B * Z
    rows = E * CAP
    top = expert_ids.shape[1]
    dma = pltpu.SemaphoreType.DMA
    vmem = pltpu.VMEM
    merged, wt = pl.pallas_call(
        functools.partial(kernel, E, B, Z),
        out_shape=(
            jax.ShapeDtypeStruct((2 * rows, W), BF16),
            jax.ShapeDtypeStruct((2 * rows, T), BF16),
        ),
        in_specs=[pl.BlockSpec(memory_space=pl.ANY)] * 6,
        out_specs=(pl.BlockSpec(memory_space=vmem), pl.BlockSpec(memory_space=vmem)),
        scratch_shapes=[
            vmem((top, T), jnp.int32),
            vmem((top, T), F32),
            vmem((T, W), BF16),
            vmem((N, W, H), BF16),
            vmem((N, W, H), BF16),
            vmem((N, H, W), BF16),
            vmem((E, CAP, W), BF16),
            vmem((N, E, CAP, W), BF16),
            vmem((rows, H), F32),
            vmem((rows, H), F32),
            vmem((B - 1, Z, rows, W), BF16),
            vmem((B - 1, Z, rows, W), BF16),
            vmem((Z, E, CAP, W), BF16),
            vmem((E, Z, CAP, W), BF16),
            dma((3,)), dma((N,)), dma((N,)), dma((N,)),
            dma((Z, E)), dma((Z, E)),
            dma((B - 1, Z)), dma((B - 1, Z)),
            dma((B - 1, Z)), dma((B - 1, Z)),
            dma((Z, E)), dma((E, Z)),
        ],
        compiler_params=pltpu.CompilerParams(collective_id=0, has_side_effects=True),
    )(expert_ids.T, route_weight.T, tokens, w_gate, w_up, w_down)
    mixed = lax.dot_general(
        wt, merged, (((0,), (0,)), ((), ())), preferred_element_type=F32
    )
    return mixed.astype(BF16)


def solution(mesh):
    in_specs = (
        P("aa", ("ba", "col")),
        P("aa", None),
        P("aa", None),
        P("aa", None, ("ba", "col")),
        P("aa", None, ("ba", "col")),
        P("aa", ("ba", "col"), None),
    )
    out_specs = P("aa", ("ba", "col"))
    body = functools.partial(shards, mesh.shape["aa"], mesh.shape["ba"], mesh.shape["col"])
    return jax.shard_map(body, mesh=mesh, in_specs=in_specs, out_specs=out_specs, check_vma=False)
```

```python
import functools

import jax
import jax.numpy as jnp
from jax import lax
from jax.experimental import pallas as pl
from jax.experimental.pallas import tpu as pltpu
from jax.sharding import PartitionSpec as P

CAP = 8
MESH = pl.DeviceIdType.MESH
F32 = jnp.float32
BF16 = jnp.bfloat16


def kernel(
    E, B, Z,
    ids_hbm, rw_hbm, tok_hbm, wg_hbm, wu_hbm, wd_hbm,
    merged_ref, wt_ref,
    ids, rw, tok, wg, wu, wd, disp, xr, acc_g, acc_u, own, part, pr, total, rr,
    in_sem, wg_sem, wu_sem, wd_sem,
    d_send, d_recv, f_send, f_recv, p_send, p_recv, r_send, r_recv,
):
    a = lax.axis_index("aa")
    c = lax.axis_index("ba")
    z = lax.axis_index("col")
    N = B * Z
    T = tok.shape[0]
    W = tok.shape[1]
    rows = E * CAP

    def at(k, n, base):
        return lax.rem(base + k, n)

    if Z == 4:
        half = z // 2
        near = [z, z + 1 - 2 * lax.rem(z, 2), 2 - half, 3 - 3 * half]
    else:
        near = [lax.rem(z + k, Z) for k in range(Z)]

    def far_first():
        order = []
        for k in list(range(2, Z))[::-1] + list(range(min(Z, 2)))[::-1]:
            for i in range(E):
                if (k, i) != (0, 0):
                    order.append((k, i))
        return order

    ins = [
        pltpu.make_async_copy(ids_hbm, ids, in_sem.at[0]),
        pltpu.make_async_copy(rw_hbm, rw, in_sem.at[1]),
        pltpu.make_async_copy(tok_hbm, tok, in_sem.at[2]),
    ]
    for copy in ins:
        copy.start()

    barrier = pltpu.get_barrier_semaphore()
    for k, i in far_first():
        pl.semaphore_signal(
            barrier, inc=1, device_id=(at(i, E, a), c, near[k]), device_id_type=MESH
        )
    for b in range(1, B):
        pl.semaphore_signal(barrier, inc=1, device_id=(a, at(b, B, c), z), device_id_type=MESH)

    chunks = [(at(b, B, c), near[k]) for k in range(Z) for b in range(B)]
    w_copies = []
    for cc, zz in chunks:
        j = cc * Z + zz
        span = pl.ds(pl.multiple_of(j * W, 128), W)
        for src, dst, sem in ((wg_hbm, wg, wg_sem), (wu_hbm, wu, wu_sem)):
            pltpu.make_async_copy(src.at[0, span, :], dst.at[j], sem.at[j]).start()
    for cc, zz in chunks:
        j = cc * Z + zz
        span = pl.ds(pl.multiple_of(j * W, 128), W)
        pltpu.make_async_copy(wd_hbm.at[0, :, span], wd.at[j], wd_sem.at[j]).start()

    ins[0].wait()
    ins[1].wait()
    expert = lax.broadcasted_iota(jnp.int32, (E, T), 0)
    counted = jnp.zeros((E, T), F32)
    shares = jnp.zeros((E, T), F32)
    for k in range(ids.shape[0]):
        match = jnp.broadcast_to(ids[k : k + 1, :], (E, T)) == expert
        counted = counted + jnp.where(match, 1.0, 0.0)
        shares = shares + jnp.where(match, jnp.broadcast_to(rw[k : k + 1, :], (E, T)), 0.0)
    earlier = lax.broadcasted_iota(jnp.int32, (T, T), 0) < lax.broadcasted_iota(
        jnp.int32, (T, T), 1
    )
    before = jnp.dot(
        counted.astype(BF16), jnp.where(earlier, 1.0, 0.0).astype(BF16), preferred_element_type=F32
    )
    slot = lax.broadcasted_iota(jnp.int32, (CAP, T), 0).astype(F32)
    placed = []
    weights = []
    for e in range(E):
        hit = jnp.broadcast_to(counted[e : e + 1, :], (CAP, T)) > 0.0
        rank = jnp.broadcast_to(before[e : e + 1, :], (CAP, T))
        one = jnp.where(hit & (rank == slot), 1.0, 0.0)
        placed.append(one)
        weights.append(one * jnp.broadcast_to(shares[e : e + 1, :], (CAP, T)))
    chooser = jnp.concatenate(placed, axis=0).astype(BF16)

    ins[2].wait()
    picked = jnp.dot(chooser, tok[...], preferred_element_type=F32)
    for e in range(E):
        disp[e] = picked[e * CAP : (e + 1) * CAP, :].astype(BF16)
    mine = c * Z + z
    xr[mine, a] = disp[a]

    pl.semaphore_wait(barrier, E * Z - 1 + B - 1)

    sends = []
    for k, i in far_first():
        aa, zz = at(i, E, a), near[k]
        copy = pltpu.make_async_remote_copy(
            src_ref=disp.at[aa], dst_ref=xr.at[mine, a],
            send_sem=d_send.at[zz, aa], recv_sem=d_recv.at[z, a],
            device_id=(aa, c, zz), device_id_type=MESH,
        )
        copy.start()
        sends.append(copy)

    weight = jnp.concatenate(weights, axis=0)
    high = weight.astype(BF16).astype(F32)
    wt_ref[...] = jnp.concatenate([high, weight - high], axis=0).T.astype(BF16)

    acc_g[...] = jnp.zeros_like(acc_g)
    acc_u[...] = jnp.zeros_like(acc_u)

    def feed(j):
        span = pl.ds(pl.multiple_of(j * W, 128), W)
        x = xr[j].astype(F32).reshape(rows, W).astype(BF16)
        pltpu.make_async_copy(wg_hbm.at[0, span, :], wg.at[j], wg_sem.at[j]).wait()
        pltpu.make_async_copy(wu_hbm.at[0, span, :], wu.at[j], wu_sem.at[j]).wait()
        acc_g[...] += jnp.dot(x, wg[j], preferred_element_type=F32)
        acc_u[...] += jnp.dot(x, wu[j], preferred_element_type=F32)

    def feed_forwarded(k):
        zz = near[k]
        for b in range(1, B):
            j = at(B - b, B, c) * Z + zz
            pltpu.make_async_remote_copy(
                src_ref=xr.at[j], dst_ref=xr.at[j],
                send_sem=f_send.at[b - 1, zz], recv_sem=f_recv.at[b - 1, zz],
                device_id=(a, at(b, B, c), z), device_id_type=MESH,
            ).wait_recv()
            feed(j)

    for k in range(Z):
        zz = near[k]
        j = c * Z + zz
        for i in range(E):
            if (k, i) != (0, 0):
                aa = at(i, E, a)
                pltpu.make_async_remote_copy(
                    src_ref=xr.at[j, aa], dst_ref=xr.at[j, aa],
                    send_sem=d_send.at[zz, aa], recv_sem=d_recv.at[zz, aa],
                    device_id=(a, at(1, B, c), z), device_id_type=MESH,
                ).wait_recv()
        for b in range(1, B):
            copy = pltpu.make_async_remote_copy(
                src_ref=xr.at[j], dst_ref=xr.at[j],
                send_sem=f_send.at[b - 1, zz], recv_sem=f_recv.at[b - 1, zz],
                device_id=(a, at(b, B, c), z), device_id_type=MESH,
            )
            copy.start()
            sends.append(copy)
        feed(j)
        if k > 0:
            feed_forwarded(k - 1)
    feed_forwarded(Z - 1)

    gate = acc_g[...]
    hidden = (gate / (1.0 + jnp.exp(-gate)) * acc_u[...]).astype(BF16)

    def down(j):
        span = pl.ds(pl.multiple_of(j * W, 128), W)
        pltpu.make_async_copy(wd_hbm.at[0, :, span], wd.at[j], wd_sem.at[j]).wait()
        return jnp.dot(hidden, wd[j], preferred_element_type=F32)

    z_order = list(range(2, Z))[::-1] + list(range(min(Z, 2)))[::-1]

    def exchange(k):
        zz = near[k]
        for b in range(1, B):
            cc = at(b, B, c)
            part[b - 1, zz] = down(cc * Z + zz).astype(BF16)
            copy = pltpu.make_async_remote_copy(
                src_ref=part.at[b - 1, zz], dst_ref=pr.at[b - 1, zz],
                send_sem=p_send.at[b - 1, zz], recv_sem=p_recv.at[b - 1, zz],
                device_id=(a, cc, z), device_id_type=MESH,
            )
            copy.start()
            sends.append(copy)

    def give_back(k, value):
        zz = near[k]
        for b in range(1, B):
            pltpu.make_async_remote_copy(
                src_ref=part.at[b - 1, zz], dst_ref=pr.at[b - 1, zz],
                send_sem=p_send.at[b - 1, zz], recv_sem=p_recv.at[b - 1, zz],
                device_id=(a, at(b, B, c), z), device_id_type=MESH,
            ).wait_recv()
            value = value + pr[b - 1, zz].astype(F32)
        for e in range(E):
            total[zz, e] = value[e * CAP : (e + 1) * CAP, :].astype(BF16)
        for i in range(E):
            aa = at(i, E, a)
            if (k, i) == (0, 0):
                rr[a, z] = total[z, a]
                continue
            copy = pltpu.make_async_remote_copy(
                src_ref=total.at[zz, aa], dst_ref=rr.at[a, z],
                send_sem=r_send.at[zz, aa], recv_sem=r_recv.at[a, z],
                device_id=(aa, c, zz), device_id_type=MESH,
            )
            copy.start()
            sends.append(copy)

    for k in z_order[:2]:
        exchange(k)
    for n, k in enumerate(z_order):
        own[...] = down(c * Z + near[k])
        if n + 2 < Z:
            exchange(z_order[n + 2])
        give_back(k, own[...])

    for k in range(Z):
        for i in range(E):
            if (k, i) != (0, 0):
                aa, zz = at(i, E, a), near[k]
                pltpu.make_async_remote_copy(
                    src_ref=rr.at[aa, zz], dst_ref=rr.at[aa, zz],
                    send_sem=r_send.at[zz, aa], recv_sem=r_recv.at[aa, zz],
                    device_id=(a, at(1, B, c), z), device_id_type=MESH,
                ).wait_recv()
    outs = []
    for e in range(E):
        value = rr[e, 0].astype(F32)
        for k in range(1, Z):
            value = value + rr[e, k].astype(F32)
        outs.append(value)
    merged = jnp.concatenate(outs, axis=0).astype(BF16)
    merged_ref[0:rows, :] = merged
    merged_ref[rows : 2 * rows, :] = merged
    for copy in sends:
        copy.wait_send()


def shards(E, B, Z, tokens, expert_ids, route_weight, w_gate, w_up, w_down):
    T, W = tokens.shape
    H = w_gate.shape[2]
    N = B * Z
    rows = E * CAP
    top = expert_ids.shape[1]
    dma = pltpu.SemaphoreType.DMA
    vmem = pltpu.VMEM
    limit = 2 * (3 * N * W * H + T * W + 8 * N * rows * W) + 4 * 1024 * 1024
    merged, wt = pl.pallas_call(
        functools.partial(kernel, E, B, Z),
        out_shape=(
            jax.ShapeDtypeStruct((2 * rows, W), BF16),
            jax.ShapeDtypeStruct((T, 2 * rows), BF16),
        ),
        in_specs=[pl.BlockSpec(memory_space=pltpu.HBM)] * 6,
        out_specs=(pl.BlockSpec(memory_space=vmem), pl.BlockSpec(memory_space=vmem)),
        scratch_shapes=[
            vmem((top, T), jnp.int32),
            vmem((top, T), F32),
            vmem((T, W), BF16),
            vmem((N, W, H), BF16),
            vmem((N, W, H), BF16),
            vmem((N, H, W), BF16),
            vmem((E, CAP, W), BF16),
            vmem((N, E, CAP, W), BF16),
            vmem((rows, H), F32),
            vmem((rows, H), F32),
            vmem((rows, W), F32),
            vmem((B - 1, Z, rows, W), BF16),
            vmem((B - 1, Z, rows, W), BF16),
            vmem((Z, E, CAP, W), BF16),
            vmem((E, Z, CAP, W), BF16),
            dma((3,)), dma((N,)), dma((N,)), dma((N,)),
            dma((Z, E)), dma((Z, E)),
            dma((B - 1, Z)), dma((B - 1, Z)),
            dma((B - 1, Z)), dma((B - 1, Z)),
            dma((Z, E)), dma((E, Z)),
        ],
        compiler_params=pltpu.CompilerParams(collective_id=0, has_side_effects=True, vmem_limit_bytes=limit),
    )(*(
        pltpu.with_memory_space_constraint(x, pltpu.HBM)
        for x in (expert_ids.T, route_weight.T, tokens, w_gate, w_up, w_down)
    ))
    return jnp.dot(wt, merged, preferred_element_type=F32).astype(BF16)


def solution(mesh):
    in_specs = (
        P("aa", ("ba", "col")),
        P("aa", None),
        P("aa", None),
        P("aa", None, ("ba", "col")),
        P("aa", None, ("ba", "col")),
        P("aa", ("ba", "col"), None),
    )
    out_specs = P("aa", ("ba", "col"))
    body = functools.partial(shards, mesh.shape["aa"], mesh.shape["ba"], mesh.shape["col"])
    return jax.shard_map(body, mesh=mesh, in_specs=in_specs, out_specs=out_specs, check_vma=False)
```

```python
import functools

import jax
import jax.numpy as jnp
from jax import lax
from jax.experimental import pallas as pl
from jax.experimental.pallas import tpu as pltpu
from jax.sharding import PartitionSpec as P

CAP = 8
MESH = pl.DeviceIdType.MESH
F32 = jnp.float32
BF16 = jnp.bfloat16


def kernel(
    E, B, Z,
    ids_hbm, rw_hbm, tok_hbm, wg_hbm, wu_hbm, wd_hbm,
    merged_ref, wt_ref,
    ids, rw, tok, wg, wu, wd, disp, xr, acc_g, acc_u, own, part, pr, total, rr,
    in_sem, wg_sem, wu_sem, wd_sem,
    d_send, d_recv, f_send, f_recv, p_send, p_recv, r_send, r_recv,
):
    a = lax.axis_index("aa")
    c = lax.axis_index("ba")
    z = lax.axis_index("col")
    N = B * Z
    T = tok.shape[0]
    W = tok.shape[1]
    rows = E * CAP

    def at(k, n, base):
        return lax.rem(base + k, n)

    if Z == 4:
        half = z // 2
        near = [z, z + 1 - 2 * lax.rem(z, 2), 2 - half, 3 - 3 * half]
    else:
        near = [lax.rem(z + k, Z) for k in range(Z)]

    def peers():
        order = []
        for k in list(range(Z)):
            for i in range(E)[::-1]:
                if (k, i) != (0, 0):
                    order.append((k, i))
        return order

    ins = [
        pltpu.make_async_copy(ids_hbm, ids, in_sem.at[0]),
        pltpu.make_async_copy(rw_hbm, rw, in_sem.at[1]),
        pltpu.make_async_copy(tok_hbm, tok, in_sem.at[2]),
    ]
    for copy in ins:
        copy.start()

    barrier = pltpu.get_barrier_semaphore()
    for k, i in peers():
        pl.semaphore_signal(
            barrier, inc=1, device_id=(at(i, E, a), c, near[k]), device_id_type=MESH
        )
    for b in range(1, B):
        pl.semaphore_signal(barrier, inc=1, device_id=(a, at(b, B, c), z), device_id_type=MESH)

    chunks = [(at(b, B, c), near[k]) for k in range(Z) for b in range(B)]
    w_copies = []
    for cc, zz in chunks:
        j = cc * Z + zz
        span = pl.ds(pl.multiple_of(j * W, 128), W)
        for src, dst, sem in ((wg_hbm, wg, wg_sem), (wu_hbm, wu, wu_sem)):
            pltpu.make_async_copy(src.at[0, span, :], dst.at[j], sem.at[j]).start()
    for cc, zz in chunks:
        j = cc * Z + zz
        span = pl.ds(pl.multiple_of(j * W, 128), W)
        pltpu.make_async_copy(wd_hbm.at[0, :, span], wd.at[j], wd_sem.at[j]).start()

    ins[0].wait()
    ins[1].wait()
    expert = lax.broadcasted_iota(jnp.int32, (E, T), 0)
    counted = jnp.zeros((E, T), F32)
    shares = jnp.zeros((E, T), F32)
    for k in range(ids.shape[0]):
        match = jnp.broadcast_to(ids[k : k + 1, :], (E, T)) == expert
        counted = counted + jnp.where(match, 1.0, 0.0)
        shares = shares + jnp.where(match, jnp.broadcast_to(rw[k : k + 1, :], (E, T)), 0.0)
    earlier = lax.broadcasted_iota(jnp.int32, (T, T), 0) < lax.broadcasted_iota(
        jnp.int32, (T, T), 1
    )
    before = jnp.dot(
        counted.astype(BF16), jnp.where(earlier, 1.0, 0.0).astype(BF16), preferred_element_type=F32
    )
    slot = lax.broadcasted_iota(jnp.int32, (CAP, T), 0).astype(F32)
    placed = []
    weights = []
    for e in range(E):
        hit = jnp.broadcast_to(counted[e : e + 1, :], (CAP, T)) > 0.0
        rank = jnp.broadcast_to(before[e : e + 1, :], (CAP, T))
        one = jnp.where(hit & (rank == slot), 1.0, 0.0)
        placed.append(one)
        weights.append(one * jnp.broadcast_to(shares[e : e + 1, :], (CAP, T)))
    chooser = jnp.concatenate(placed, axis=0).astype(BF16)

    ins[2].wait()
    picked = jnp.dot(chooser, tok[...], preferred_element_type=F32)
    for e in range(E):
        disp[e] = picked[e * CAP : (e + 1) * CAP, :].astype(BF16)
    mine = c * Z + z
    xr[mine, a] = disp[a]

    pl.semaphore_wait(barrier, E * Z - 1 + B - 1)

    sends = []
    for k, i in peers():
        aa, zz = at(i, E, a), near[k]
        copy = pltpu.make_async_remote_copy(
            src_ref=disp.at[aa], dst_ref=xr.at[mine, a],
            send_sem=d_send.at[zz, aa], recv_sem=d_recv.at[z, a],
            device_id=(aa, c, zz), device_id_type=MESH,
        )
        copy.start()
        sends.append(copy)

    weight = jnp.concatenate(weights, axis=0)
    high = weight.astype(BF16).astype(F32)
    wt_ref[...] = jnp.concatenate([high, weight - high], axis=0).T.astype(BF16)

    acc_g[...] = jnp.zeros_like(acc_g)
    acc_u[...] = jnp.zeros_like(acc_u)

    def feed(j):
        span = pl.ds(pl.multiple_of(j * W, 128), W)
        x = xr[j].astype(F32).reshape(rows, W).astype(BF16)
        pltpu.make_async_copy(wg_hbm.at[0, span, :], wg.at[j], wg_sem.at[j]).wait()
        pltpu.make_async_copy(wu_hbm.at[0, span, :], wu.at[j], wu_sem.at[j]).wait()
        acc_g[...] += jnp.dot(x, wg[j], preferred_element_type=F32)
        acc_u[...] += jnp.dot(x, wu[j], preferred_element_type=F32)

    def feed_forwarded(k):
        zz = near[k]
        for b in range(1, B):
            j = at(B - b, B, c) * Z + zz
            pltpu.make_async_remote_copy(
                src_ref=xr.at[j], dst_ref=xr.at[j],
                send_sem=f_send.at[b - 1, zz], recv_sem=f_recv.at[b - 1, zz],
                device_id=(a, at(b, B, c), z), device_id_type=MESH,
            ).wait_recv()
            feed(j)

    for k in range(Z):
        zz = near[k]
        j = c * Z + zz
        for i in range(E):
            if (k, i) != (0, 0):
                aa = at(i, E, a)
                pltpu.make_async_remote_copy(
                    src_ref=xr.at[j, aa], dst_ref=xr.at[j, aa],
                    send_sem=d_send.at[zz, aa], recv_sem=d_recv.at[zz, aa],
                    device_id=(a, at(1, B, c), z), device_id_type=MESH,
                ).wait_recv()
        for b in range(1, B):
            copy = pltpu.make_async_remote_copy(
                src_ref=xr.at[j], dst_ref=xr.at[j],
                send_sem=f_send.at[b - 1, zz], recv_sem=f_recv.at[b - 1, zz],
                device_id=(a, at(b, B, c), z), device_id_type=MESH,
            )
            copy.start()
            sends.append(copy)
        feed(j)
        if k > 0:
            feed_forwarded(k - 1)
    feed_forwarded(Z - 1)

    gate = acc_g[...]
    hidden = (gate / (1.0 + jnp.exp(-gate)) * acc_u[...]).astype(BF16)

    def down(j):
        span = pl.ds(pl.multiple_of(j * W, 128), W)
        pltpu.make_async_copy(wd_hbm.at[0, :, span], wd.at[j], wd_sem.at[j]).wait()
        return jnp.dot(hidden, wd[j], preferred_element_type=F32)

    z_order = list(range(2, Z))[::-1] + list(range(min(Z, 2)))[::-1]

    def exchange(k):
        zz = near[k]
        for b in range(1, B):
            cc = at(b, B, c)
            part[b - 1, zz] = down(cc * Z + zz).astype(BF16)
            copy = pltpu.make_async_remote_copy(
                src_ref=part.at[b - 1, zz], dst_ref=pr.at[b - 1, zz],
                send_sem=p_send.at[b - 1, zz], recv_sem=p_recv.at[b - 1, zz],
                device_id=(a, cc, z), device_id_type=MESH,
            )
            copy.start()
            sends.append(copy)

    def give_back(k, value):
        zz = near[k]
        for b in range(1, B):
            pltpu.make_async_remote_copy(
                src_ref=part.at[b - 1, zz], dst_ref=pr.at[b - 1, zz],
                send_sem=p_send.at[b - 1, zz], recv_sem=p_recv.at[b - 1, zz],
                device_id=(a, at(b, B, c), z), device_id_type=MESH,
            ).wait_recv()
            value = value + pr[b - 1, zz].astype(F32)
        for e in range(E):
            total[zz, e] = value[e * CAP : (e + 1) * CAP, :].astype(BF16)
        for i in range(E)[::-1]:
            aa = at(i, E, a)
            if (k, i) == (0, 0):
                rr[a, z] = total[z, a]
                continue
            copy = pltpu.make_async_remote_copy(
                src_ref=total.at[zz, aa], dst_ref=rr.at[a, z],
                send_sem=r_send.at[zz, aa], recv_sem=r_recv.at[a, z],
                device_id=(aa, c, zz), device_id_type=MESH,
            )
            copy.start()
            sends.append(copy)

    for k in z_order[:1]:
        exchange(k)
    for n, k in enumerate(z_order):
        own[...] = down(c * Z + near[k])
        if n + 1 < Z:
            exchange(z_order[n + 1])
        give_back(k, own[...])

    for k in range(Z):
        for i in range(E):
            if (k, i) != (0, 0):
                aa, zz = at(i, E, a), near[k]
                pltpu.make_async_remote_copy(
                    src_ref=rr.at[aa, zz], dst_ref=rr.at[aa, zz],
                    send_sem=r_send.at[zz, aa], recv_sem=r_recv.at[aa, zz],
                    device_id=(a, at(1, B, c), z), device_id_type=MESH,
                ).wait_recv()
    outs = []
    for e in range(E):
        value = rr[e, 0].astype(F32)
        for k in range(1, Z):
            value = value + rr[e, k].astype(F32)
        outs.append(value)
    merged = jnp.concatenate(outs, axis=0).astype(BF16)
    merged_ref[0:rows, :] = merged
    merged_ref[rows : 2 * rows, :] = merged
    for copy in sends:
        copy.wait_send()


def shards(E, B, Z, tokens, expert_ids, route_weight, w_gate, w_up, w_down):
    T, W = tokens.shape
    H = w_gate.shape[2]
    N = B * Z
    rows = E * CAP
    top = expert_ids.shape[1]
    dma = pltpu.SemaphoreType.DMA
    vmem = pltpu.VMEM
    limit = 2 * (3 * N * W * H + T * W + 8 * N * rows * W) + 4 * 1024 * 1024
    merged, wt = pl.pallas_call(
        functools.partial(kernel, E, B, Z),
        out_shape=(
            jax.ShapeDtypeStruct((2 * rows, W), BF16),
            jax.ShapeDtypeStruct((T, 2 * rows), BF16),
        ),
        in_specs=[pl.BlockSpec(memory_space=pltpu.HBM)] * 6,
        out_specs=(pl.BlockSpec(memory_space=vmem), pl.BlockSpec(memory_space=vmem)),
        scratch_shapes=[
            vmem((top, T), jnp.int32),
            vmem((top, T), F32),
            vmem((T, W), BF16),
            vmem((N, W, H), BF16),
            vmem((N, W, H), BF16),
            vmem((N, H, W), BF16),
            vmem((E, CAP, W), BF16),
            vmem((N, E, CAP, W), BF16),
            vmem((rows, H), F32),
            vmem((rows, H), F32),
            vmem((rows, W), F32),
            vmem((B - 1, Z, rows, W), BF16),
            vmem((B - 1, Z, rows, W), BF16),
            vmem((Z, E, CAP, W), BF16),
            vmem((E, Z, CAP, W), BF16),
            dma((3,)), dma((N,)), dma((N,)), dma((N,)),
            dma((Z, E)), dma((Z, E)),
            dma((B - 1, Z)), dma((B - 1, Z)),
            dma((B - 1, Z)), dma((B - 1, Z)),
            dma((Z, E)), dma((E, Z)),
        ],
        compiler_params=pltpu.CompilerParams(collective_id=0, has_side_effects=True, vmem_limit_bytes=limit),
    )(*(
        pltpu.with_memory_space_constraint(x, pltpu.HBM)
        for x in (expert_ids.T, route_weight.T, tokens, w_gate, w_up, w_down)
    ))
    return jnp.dot(wt, merged, preferred_element_type=F32).astype(BF16)


def solution(mesh):
    in_specs = (
        P("aa", ("ba", "col")),
        P("aa", None),
        P("aa", None),
        P("aa", None, ("ba", "col")),
        P("aa", None, ("ba", "col")),
        P("aa", ("ba", "col"), None),
    )
    out_specs = P("aa", ("ba", "col"))
    body = functools.partial(shards, mesh.shape["aa"], mesh.shape["ba"], mesh.shape["col"])
    return jax.shard_map(body, mesh=mesh, in_specs=in_specs, out_specs=out_specs, check_vma=False)
```
